32 devices in a mesh: mol: 2 (over x), pts: 16 (over z, y, core).
Axes of the slice: x: 2, y: 2, z: 4, core: 2. Of those that a mesh axis runs over, the one named last changes fastest.
Arguments:
- points_map: bfloat16 [12800, 800], P(('mol', 'pts')), parts along dimension 0, may hold values from -0.21875 to 0.21875
- trial: bfloat16 [12800, 128], P('mol'), parts along dimension 0, may hold values from -6 to 6
- core: bfloat16 [12800, 6400], P(('mol', 'pts')), parts along dimension 0, may hold values from -2 to 4, as said below
- walkers: bfloat16 [1600, 12, 128], P('mol'), parts along dimension 0, may hold values from -6 to 6
- draws: int32 [12800, 12], P(('mol', 'pts')), parts along dimension 0, may hold values from 0 to 3
Outputs:
- new_walkers: bfloat16 [1600, 12, 128], P(('mol', 'pts')), parts along dimension 0
- energy: float32 [24], P('mol'), parts along dimension 0
The draws below stay inside these ranges and needn't reach their ends.
There are 2 independent parts, one for each index of `mol`. The reference program is written for one: setup_inputs(seed, part) draws one part's arguments, and reference() takes and returns one part's arrays. A program takes and returns all parts, laid end to end along the dimension named above; each array names one. Nothing has to cross between parts.
Inputs may be any that keep to these rules, and one draw needn't show every extreme that they name: core is symmetric.
All inputs are finite; a program needn't handle non-finite values.
Results may differ from the reference program's by a relative error of at most 0.018.
Values may be sent and summed in bfloat16 or wider, within the bound.
A program may use at most 192 MiB of HBM per device.

```python
import math
import jax
import jax.numpy as jnp
from jax import lax

N = 800
NOCC = 128
POINTS = 6400
WALKERS = 12
TAYLOR = 3


def draw_core(key, part):
    first_key = jax.random.fold_in(jax.random.fold_in(key, 11), 0)
    gauss = jax.random.normal(first_key, (POINTS, POINTS), jnp.float32)
    matrix = (gauss + gauss.T) / math.sqrt(2.0 * POINTS)
    matrix = matrix + jnp.eye(POINTS, dtype=jnp.float32)
    return matrix.astype(jnp.bfloat16)


def with_ends(drawn, key, smallest, largest):
    longest = drawn.shape.index(max(drawn.shape))
    spots = []
    for shift in (0, 1):
        where = [jax.random.randint(jax.random.fold_in(key, axis), (), 0, length) for axis, length in enumerate(drawn.shape)]
        where[longest] = (where[longest] + shift) % drawn.shape[longest]
        spots.append(tuple(where))
    return drawn.at[spots[0]].set(smallest).at[spots[1]].set(largest)


def shard_levels(stream_key, extent, pieces, least, high):
    gain, own = 1.0, jax.random.fold_in(stream_key, 6)
    for position, blocks in pieces:
        steps = jnp.exp(jax.random.uniform(jax.random.fold_in(own, position), (blocks,), jnp.float32, least / len(pieces), high / len(pieces)))
        gain = gain * jnp.repeat(steps, extent[position] // blocks).reshape([-1 if axis == position else 1 for axis in range(len(extent))])
    return gain


def scatter_about(own_key, extent, scale, bound, cuts=(), kind=jnp.bfloat16):
    loudness = shard_levels(own_key, extent, cuts, -0.22, 0.18) if cuts else 1.0
    values = jax.random.normal(own_key, extent, jnp.float32) * scale * loudness
    return jnp.minimum(jnp.maximum(values, -bound), bound).astype(kind)


def setup_inputs(seed: int = 0, part: int = 0) -> dict:
    key_list = jax.random.split(jax.random.key(seed), 6)
    own_keys = jax.random.split(jax.random.fold_in(key_list[5], part), 6)
    points_map = scatter_about(own_keys[0], (POINTS, N), N ** -0.5, 0.21875, ((0, 16),))
    trial = scatter_about(own_keys[1], (POINTS, NOCC), 1.0, 6.0)
    core = draw_core(jax.random.fold_in(jax.random.fold_in(key_list[5], part), 71), part)
    walkers = scatter_about(own_keys[3], (N, WALKERS, NOCC), 1.0, 6.0)
    draws = with_ends(jax.random.randint(own_keys[4], (POINTS, WALKERS), 0, 4), jax.random.fold_in(own_keys[4], 1), 0, 3).astype(jnp.int32)
    return dict(points_map=points_map, trial=trial, core=core, walkers=walkers, draws=draws)


GAUSS_NODES = (-2.3344142, -0.7419637, 0.7419637, 2.3344142)
FIELD_STEP = 0.15

def node_lookup(draws):
    values = jnp.zeros(draws.shape, jnp.float32)
    for number, node in enumerate(GAUSS_NODES):
        values = values + jnp.where(draws == number, node, 0.0).astype(jnp.float32)
    return values

def reference(points_map, trial, core, walkers, draws):
    flat_walkers = walkers.reshape(N, WALKERS * NOCC)
    orbit = jnp.dot(points_map, flat_walkers, preferred_element_type=jnp.float32).astype(jnp.bfloat16).reshape(POINTS, WALKERS, NOCC)
    density = (lax.optimization_barrier(jnp.sum(orbit.astype(jnp.float32) * trial.astype(jnp.float32)[:, None, :], axis=2)) / math.sqrt(NOCC)).astype(jnp.bfloat16)
    potential = jnp.dot(core, density, preferred_element_type=jnp.float32)
    field = FIELD_STEP * (node_lookup(draws) - FIELD_STEP * potential)
    running = walkers.astype(jnp.float32)
    current = orbit
    term_now = walkers
    for degree in range(1, TAYLOR + 1):
        if degree > 1:
            current = jnp.dot(points_map, term_now.reshape(N, WALKERS * NOCC), preferred_element_type=jnp.float32).astype(jnp.bfloat16).reshape(POINTS, WALKERS, NOCC)
        scaled = (field[:, :, None] * current.astype(jnp.float32)).astype(jnp.bfloat16).reshape(POINTS, WALKERS * NOCC)
        summed = jnp.einsum('pi,pc->ic', points_map.astype(jnp.float32), scaled.astype(jnp.float32))
        term_now = (summed / degree).astype(jnp.bfloat16).reshape(N, WALKERS, NOCC)
        running = running + term_now.astype(jnp.float32)
    new_walkers = running.astype(jnp.bfloat16)
    hartree = lax.optimization_barrier(jnp.sum(density.astype(jnp.float32) * potential, axis=0))
    core_wide = core.astype(jnp.float32)

    def per_walker(orbit_walker):
        mixed = jnp.dot(orbit_walker, trial.T, preferred_element_type=jnp.float32)
        return jnp.sum(core_wide * mixed * mixed.T) / NOCC
    exchange = lax.map(per_walker, jnp.moveaxis(orbit, 1, 0))
    energy = (hartree - exchange) / (2.0 * POINTS)
    return (new_walkers, energy)
```

```python
import functools
import math

import jax
import jax.numpy as jnp
from jax import lax
from jax.experimental import pallas as pl
from jax.experimental.pallas import tpu as pltpu
from jax.sharding import PartitionSpec as P

TAYLOR = 3


GAUSS_NODES = (-2.3344142, -0.7419637, 0.7419637, 2.3344142)
FIELD_STEP = 0.15
LANES = 128
CONTRACT_LAST = (((1,), (1,)), ((), ()))
CONTRACT_FIRST = (((0,), (0,)), ((), ()))


def node_lookup(draws):
    values = jnp.zeros(draws.shape, jnp.float32)
    for number, node in enumerate(GAUSS_NODES):
        values = values + jnp.where(draws == number, node, 0.0).astype(jnp.float32)
    return values


def dot(left, right, dims):
    return lax.dot_general(left, right, dims, preferred_element_type=jnp.float32)


def exchange_kernel(n, walker_count, map_ref, trial_ref, trial_own, core_ref, walkers_ref, orbit_own, out_ref, blocks):
    rows, occupied = trial_own.shape
    window = blocks.shape[0]
    step = pl.program_id(0)
    me = lax.axis_index("pts")
    block = lax.rem(me + step, n)
    first = block * rows
    base = pl.multiple_of(first // LANES * LANES, LANES)
    shift = pl.multiple_of(first - base, 16)

    @pl.when(step == 0)
    def _():
        out_ref[...] = jnp.zeros_like(out_ref)

    blocks[...] = jnp.zeros_like(blocks)
    weight = jnp.where(jnp.logical_or(step == 0, 2 * step == n), 1.0, 2.0)
    blocks[pl.ds(shift, rows), :] = dot(
        map_ref[0], walkers_ref[...], (((1,), (0,)), ((), ()))
    ).astype(jnp.bfloat16)
    core_here = core_ref[:, pl.ds(base, window)].astype(jnp.float32)
    trial_there = trial_ref[pl.ds(base, window), :]
    for walker in range(walker_count):
        cols = slice(walker * occupied, (walker + 1) * occupied)
        forward = dot(orbit_own[:, cols], trial_there, CONTRACT_LAST)
        backward = dot(trial_own[...], blocks[:, cols], CONTRACT_LAST)
        product = core_here * forward * backward
        out_ref[walker] += weight * jnp.sum(product.reshape(rows // 8, 8, window), axis=0)


def exchange_sums(n, walker_count, map_full, trial, trial_here, core, flat_walkers, orbit):
    rows, orbitals = map_full.shape[0] // n, map_full.shape[1]
    columns = flat_walkers.shape[1]
    window = (rows + (LANES - 16) + LANES - 1) // LANES * LANES
    steps = n // 2 + 1
    whole = lambda a: pl.BlockSpec(a.shape, lambda s: (0,) * a.ndim)
    flops = 2 * steps * (rows * orbitals * columns + 2 * rows * window * columns)
    return pl.pallas_call(
        functools.partial(exchange_kernel, n, walker_count),
        grid=(steps,),
        out_shape=jax.ShapeDtypeStruct((walker_count, 8, window), jnp.float32),
        in_specs=[
            pl.BlockSpec((1, rows, orbitals), lambda s: (lax.rem(lax.axis_index("pts") + s, n), 0, 0)),
            whole(trial),
            whole(trial_here),
            whole(core),
            whole(flat_walkers),
            whole(orbit),
        ],
        out_specs=pl.BlockSpec((walker_count, 8, window), lambda s: (0, 0, 0)),
        scratch_shapes=[pltpu.VMEM((window, columns), jnp.bfloat16)],
        cost_estimate=pl.CostEstimate(flops=flops, bytes_accessed=2 * map_full.size, transcendentals=0),
        compiler_params=pltpu.CompilerParams(vmem_limit_bytes=60 * 2**20),
        name="exchange",
    )(map_full.reshape(n, rows, orbitals), trial, trial_here, core, flat_walkers, orbit)


def propagate_kernel(n, occupied, piece, map_ref, field_ref, cols_ref, out_ref, wide, total, term):
    points, orbitals = map_ref.shape
    own = cols_ref.shape[0]
    start = lax.axis_index("pts") * own
    walker_ids = (start + lax.broadcasted_iota(jnp.int32, (1, own), 1)) // occupied
    low = start // occupied
    span = (own + occupied - 2) // occupied + 1
    running = cols_ref[...].astype(jnp.float32)
    term[...] = cols_ref[...]
    for degree in range(1, TAYLOR + 1):
        total[...] = jnp.zeros_like(total)

        @pl.loop(0, points // piece)
        def _(number):
            here = pl.ds(pl.multiple_of(number * piece, piece), piece)
            if degree == 1:
                field = field_ref[here, :]
                lane = lax.broadcasted_iota(jnp.int32, field.shape, 1)
                spread = jnp.zeros((piece, own), jnp.float32)
                for offset in range(span):
                    column = jnp.sum(jnp.where(lane == low + offset, field, 0.0), axis=1, keepdims=True)
                    spread = jnp.where(walker_ids == low + offset, column, spread)
                wide[here, :] = spread
            block = map_ref[here, :]
            current = dot(block, term[...], CONTRACT_LAST).astype(jnp.bfloat16)
            scaled = (wide[here, :] * current.astype(jnp.float32)).astype(jnp.bfloat16)
            total[...] += dot(scaled, block, CONTRACT_FIRST)

        term[...] = (total[...] / degree).astype(jnp.bfloat16)
        running = running + term[...].astype(jnp.float32)
    out_ref[...] = running.astype(jnp.bfloat16)


def propagate(n, occupied, map_full, field_full, own_cols_t):
    points, orbitals = map_full.shape
    own = own_cols_t.shape[0]
    piece = next(p for p in (1280, 640, 256, points // n) if points % p == 0)
    return pl.pallas_call(
        functools.partial(propagate_kernel, n, occupied, piece),
        out_shape=jax.ShapeDtypeStruct((own, orbitals), jnp.bfloat16),
        in_specs=[pl.BlockSpec(memory_space=pltpu.VMEM)] * 3,
        out_specs=pl.BlockSpec(memory_space=pltpu.VMEM),
        scratch_shapes=[
            pltpu.VMEM((points, own), jnp.float32),
            pltpu.VMEM((own, orbitals), jnp.float32),
            pltpu.VMEM((own, orbitals), jnp.bfloat16),
        ],
        cost_estimate=pl.CostEstimate(
            flops=12 * points * orbitals * own, bytes_accessed=2 * map_full.size, transcendentals=0
        ),
        compiler_params=pltpu.CompilerParams(vmem_limit_bytes=60 * 2**20),
        name="propagate",
    )(map_full, field_full, own_cols_t)


def exchange_plain(trial, trial_here, core, orbit):
    core_block = core.astype(jnp.float32)

    def per_walker(operands):
        left_orb, right_orb = operands
        forward = jnp.dot(left_orb, trial.T, preferred_element_type=jnp.float32)
        backward = jnp.dot(trial_here, right_orb.T, preferred_element_type=jnp.float32)
        return jnp.sum(core_block * forward * backward)

    everyone = lax.all_gather(orbit, "pts", axis=0, tiled=True)
    return lax.map(per_walker, (jnp.moveaxis(orbit, 1, 0), jnp.moveaxis(everyone, 1, 0)))


def body(points_map, trial, core, walkers, draws):
    point_rows = points_map.shape[0]
    orbitals = points_map.shape[1]
    walker_count = walkers.shape[1]
    occupied = walkers.shape[2]
    n = lax.axis_size("pts")
    map_full = lax.all_gather(points_map, "pts", axis=0, tiled=True)
    point_first = lax.axis_index("pts") * point_rows
    trial_here = lax.dynamic_slice_in_dim(trial, point_first, point_rows, 0)
    flat_walkers = walkers.reshape(orbitals, walker_count * occupied)
    flat_orbit = jnp.dot(points_map, flat_walkers, preferred_element_type=jnp.float32).astype(jnp.bfloat16)
    orbit = flat_orbit.reshape(point_rows, walker_count, occupied)
    density = (
        jnp.sum(orbit.astype(jnp.float32) * trial_here.astype(jnp.float32)[:, None, :], axis=2)
        / math.sqrt(occupied)
    ).astype(jnp.bfloat16)
    potential = jnp.dot(
        core,
        lax.all_gather(density, "pts", axis=0, tiled=True),
        preferred_element_type=jnp.float32,
    )
    field = FIELD_STEP * (node_lookup(draws) - FIELD_STEP * potential)
    field_full = lax.all_gather(field, "pts", axis=0, tiled=True)
    own_rows = orbitals // n
    own_cols = walker_count * occupied // n
    col_start = lax.axis_index("pts") * own_cols
    cols_walkers = lax.dynamic_slice_in_dim(flat_walkers, col_start, own_cols, 1)
    final_t = propagate(n, occupied, map_full, field_full, cols_walkers.T)
    placed = lax.all_to_all(final_t.T, "pts", split_axis=0, concat_axis=1, tiled=True)
    if point_rows % 16 == 0 and n % 2 == 0:
        exchange = jnp.sum(
            exchange_sums(n, walker_count, map_full, trial, trial_here, core, flat_walkers, flat_orbit),
            axis=(1, 2),
        )
    else:
        exchange = exchange_plain(trial, trial_here, core, orbit)
    hartree = jnp.sum(density.astype(jnp.float32) * potential, axis=0)
    total_points = point_rows * n
    energy = lax.psum((hartree - exchange / occupied) / (2.0 * total_points), "pts")
    return (placed.reshape(own_rows, walker_count, occupied), energy)


def solution(mesh):
    placed = (
        P(("mol", "pts"), None),
        P("mol", None),
        P(("mol", "pts"), None),
        P("mol", None, None),
        P(("mol", "pts"), None),
    )
    return jax.shard_map(
        body,
        mesh=mesh,
        in_specs=placed,
        out_specs=(P(("mol", "pts"), None, None), P("mol")),
        check_vma=False,
    )
```

```python
import functools
import math

import jax
import jax.numpy as jnp
from jax import lax
from jax.experimental import pallas as pl
from jax.experimental.pallas import tpu as pltpu
from jax.sharding import PartitionSpec as P

TAYLOR = 3


GAUSS_NODES = (-2.3344142, -0.7419637, 0.7419637, 2.3344142)
FIELD_STEP = 0.15
LANES = 128
CONTRACT_LAST = (((1,), (1,)), ((), ()))
CONTRACT_FIRST = (((0,), (0,)), ((), ()))


def node_lookup(draws):
    values = jnp.zeros(draws.shape, jnp.float32)
    for number, node in enumerate(GAUSS_NODES):
        values = values + jnp.where(draws == number, node, 0.0).astype(jnp.float32)
    return values


def dot(left, right, dims):
    return lax.dot_general(left, right, dims, preferred_element_type=jnp.float32)


def add_exchange(out_ref, blocks, map_block, trial_ref, trial_own, core_ref, walkers_ref, orbit_own, first, weight):
    rows, occupied = trial_own.shape
    window = blocks.shape[0]
    base = pl.multiple_of(first // LANES * LANES, LANES)
    shift = pl.multiple_of(first - base, 16)
    blocks[...] = jnp.zeros_like(blocks)
    blocks[pl.ds(shift, rows), :] = dot(map_block, walkers_ref[...], (((1,), (0,)), ((), ()))).astype(jnp.bfloat16)
    core_here = core_ref[:, pl.ds(base, window)].astype(jnp.float32)
    trial_there = trial_ref[pl.ds(base, window), :]
    for walker in range(out_ref.shape[0]):
        cols = slice(walker * occupied, (walker + 1) * occupied)
        forward = dot(orbit_own[:, cols], trial_there, CONTRACT_LAST)
        backward = dot(trial_own[...], blocks[:, cols], CONTRACT_LAST)
        product = core_here * forward * backward
        out_ref[walker] += weight * jnp.sum(product.reshape(rows // 8, 8, window), axis=0)


def spread_field(field_ref, here, piece, start, own, occupied):
    walker_ids = (start + lax.broadcasted_iota(jnp.int32, (1, own), 1)) // occupied
    low = start // occupied
    field = field_ref[here, :]
    lane = lax.broadcasted_iota(jnp.int32, field.shape, 1)
    spread = jnp.zeros((piece, own), jnp.float32)
    for offset in range((own + occupied - 2) // occupied + 1):
        column = jnp.sum(jnp.where(lane == low + offset, field, 0.0), axis=1, keepdims=True)
        spread = jnp.where(walker_ids == low + offset, column, spread)
    return spread


def fused_kernel(
    n, piece, own_map, trial_ref, trial_own, core_ref, walkers_ref, orbit_own, field_ref, cols_ref,
    sums_ref, out_ref,
    blocks, gathered, wide, total, term, right_sems, left_sems, side_sems, recv_sems,
):
    rows, occupied = trial_own.shape
    own = cols_ref.shape[0]
    points = gathered.shape[0]
    chips = n // 2
    far = chips // 2
    top = (rows // 2 + 15) // 16 * 16
    parts = ((0, top), (top, rows - top))
    me = lax.axis_index("pts")
    core_id = lax.rem(me, 2)
    chip = me // 2
    ring = jnp.where(lax.rem(chip, 2) == 0, chip // 2, chips - 1 - chip // 2)

    def device(place, side):
        place = lax.rem(place + 2 * chips, chips)
        where = jnp.where(place < far, 2 * place, 2 * (chips - 1 - place) + 1)
        return 2 * where + side

    right, left, partner = device(ring + 1, core_id), device(ring - 1, core_id), device(ring, 1 - core_id)

    def slot(index, part=None):
        offset, length = (0, rows) if part is None else parts[part]
        return gathered.at[pl.ds(pl.multiple_of(index * rows + offset, 16), length), :]

    def send(src, index, part, send_sem, target):
        return pltpu.make_async_remote_copy(
            src_ref=src,
            dst_ref=slot(index, part),
            send_sem=send_sem,
            recv_sem=recv_sems.at[index, part or 0],
            device_id={"pts": target},
            device_id_type=pl.DeviceIdType.MESH,
        )

    def forward(index, part, send_sem, target):
        send(slot(index, part), index, part, send_sem, target).start()

    def arrived(index, part=None):
        send(slot(index, part), index, part, side_sems.at[0, 0], partner).wait_recv()

    barrier = pltpu.get_barrier_semaphore()
    for other in (right, left, partner):
        pl.semaphore_signal(barrier, inc=1, device_id={"pts": other}, device_id_type=pl.DeviceIdType.MESH)
    pl.semaphore_wait(barrier, 3)
    send(own_map, me, None, right_sems.at[0], right).start()
    send(own_map, me, None, left_sems.at[0], left).start()
    send(own_map, me, None, side_sems.at[0, 0], partner).start()
    gathered[pl.ds(pl.multiple_of(me * rows, 16), rows), :] = own_map[...]
    sums_ref[...] = jnp.zeros_like(sums_ref)
    total[...] = jnp.zeros_like(total)
    term[...] = cols_ref[...]

    def add_block(index):
        here = pl.ds(pl.multiple_of(index * rows, 16), rows)
        block = gathered[here, :]
        spread = spread_field(field_ref, here, rows, me * own, own, occupied)
        wide[here, :] = spread
        current = dot(block, term[...], CONTRACT_LAST).astype(jnp.bfloat16)
        scaled = (spread * current.astype(jnp.float32)).astype(jnp.bfloat16)
        total[...] += dot(scaled, block, CONTRACT_FIRST)

    @pl.loop(0, 2 * far + 1)
    def _(task):
        hop = task // 2
        same = lax.rem(task, 2) == 0
        ahead, behind = device(ring + hop, core_id), device(ring - hop, core_id)
        ahead_side, behind_side = device(ring + hop, 1 - core_id), device(ring - hop, 1 - core_id)
        last = hop == far
        middle = jnp.logical_and(hop > 0, hop < far)

        @pl.when(jnp.logical_and(same, middle))
        def _():
            arrived(behind)

            @pl.when(hop < far - 1)
            def _():
                forward(behind, None, right_sems.at[hop], right)

            @pl.when(hop == far - 1)
            def _():
                forward(behind, 0, right_sems.at[hop], right)

            forward(behind, None, side_sems.at[0, hop], partner)
            arrived(ahead)

            @pl.when(hop < far - 1)
            def _():
                forward(ahead, None, left_sems.at[hop], left)

            @pl.when(hop == far - 1)
            def _():
                forward(ahead, 1, left_sems.at[hop], left)

            forward(ahead, None, side_sems.at[1, hop], partner)

        @pl.when(last)
        def _():
            for part in range(2):
                arrived(ahead, part)
                forward(ahead, part, side_sems.at[part, hop], partner)
            for part in range(2):
                arrived(ahead_side, part)

        @pl.when(jnp.logical_not(same))
        def _():
            arrived(ahead_side)

            @pl.when(hop > 0)
            def _():
                arrived(behind_side)

        near = jnp.where(same, ahead, ahead_side)
        opposite = jnp.where(last, ahead_side, jnp.where(same, behind, behind_side))
        pair = jnp.where(jnp.logical_and(last, ring >= far), ahead_side, near)
        add_exchange(
            sums_ref, blocks, gathered[pl.ds(pl.multiple_of(pair * rows, 16), rows), :], trial_ref, trial_own,
            core_ref, walkers_ref, orbit_own, pair * rows, jnp.where(hop == 0, 1.0, 2.0),
        )
        add_block(near)

        @pl.when(hop > 0)
        def _():
            add_block(opposite)

    running = cols_ref[...].astype(jnp.float32)
    for degree in range(1, TAYLOR + 1):
        if degree > 1:
            total[...] = jnp.zeros_like(total)

            @pl.loop(0, points // piece)
            def _(number):
                here = pl.ds(pl.multiple_of(number * piece, piece), piece)
                block = gathered[here, :]
                current = dot(block, term[...], CONTRACT_LAST).astype(jnp.bfloat16)
                scaled = (wide[here, :] * current.astype(jnp.float32)).astype(jnp.bfloat16)
                total[...] += dot(scaled, block, CONTRACT_FIRST)

        term[...] = (total[...] / degree).astype(jnp.bfloat16)
        running = running + term[...].astype(jnp.float32)
    out_ref[...] = running.astype(jnp.bfloat16)

    for hop in range(far):
        for number, (sems, target) in enumerate(((right_sems, right), (left_sems, left))):
            part = number if hop == far - 1 and hop > 0 else None
            send(slot(me, part), me, part, sems.at[hop], target).wait_send()
    send(slot(me), me, None, side_sems.at[0, 0], partner).wait_send()
    for hop in range(1, far + 1):
        for number in range(2):
            part = number if hop == far else None
            send(slot(me, part), me, part, side_sems.at[number, hop], partner).wait_send()


def fused(n, points_map, trial, trial_here, core, flat_walkers, orbit, field_full, own_cols_t, walker_count):
    rows, orbitals = points_map.shape
    points, own, columns = rows * n, own_cols_t.shape[0], flat_walkers.shape[1]
    window = (rows + (LANES - 16) + LANES - 1) // LANES * LANES
    far = n // 4
    piece = next(p for p in (1280, 640, 256, rows) if points % p == 0)
    dma = pltpu.SemaphoreType.DMA
    return pl.pallas_call(
        functools.partial(fused_kernel, n, piece),
        out_shape=(
            jax.ShapeDtypeStruct((walker_count, 8, window), jnp.float32),
            jax.ShapeDtypeStruct((own, orbitals), jnp.bfloat16),
        ),
        in_specs=[pl.BlockSpec(memory_space=pltpu.VMEM)] * 8,
        out_specs=[pl.BlockSpec(memory_space=pltpu.VMEM)] * 2,
        scratch_shapes=[
            pltpu.VMEM((window, columns), jnp.bfloat16),
            pltpu.VMEM((points, orbitals), jnp.bfloat16),
            pltpu.VMEM((points, own), jnp.float32),
            pltpu.VMEM((own, orbitals), jnp.float32),
            pltpu.VMEM((own, orbitals), jnp.bfloat16),
            dma((far,)),
            dma((far,)),
            dma((2, far + 1)),
            dma((n, 2)),
        ],
        compiler_params=pltpu.CompilerParams(
            collective_id=0, has_side_effects=True, vmem_limit_bytes=60 * 2**20
        ),
        name="fused",
    )(points_map, trial, trial_here, core, flat_walkers, orbit, field_full, own_cols_t)


def propagate_kernel(n, occupied, piece, map_ref, field_ref, cols_ref, out_ref, wide, total, term):
    points, orbitals = map_ref.shape
    own = cols_ref.shape[0]
    start = lax.axis_index("pts") * own
    walker_ids = (start + lax.broadcasted_iota(jnp.int32, (1, own), 1)) // occupied
    low = start // occupied
    span = (own + occupied - 2) // occupied + 1
    running = cols_ref[...].astype(jnp.float32)
    term[...] = cols_ref[...]
    for degree in range(1, TAYLOR + 1):
        total[...] = jnp.zeros_like(total)

        @pl.loop(0, points // piece)
        def _(number):
            here = pl.ds(pl.multiple_of(number * piece, piece), piece)
            if degree == 1:
                field = field_ref[here, :]
                lane = lax.broadcasted_iota(jnp.int32, field.shape, 1)
                spread = jnp.zeros((piece, own), jnp.float32)
                for offset in range(span):
                    column = jnp.sum(jnp.where(lane == low + offset, field, 0.0), axis=1, keepdims=True)
                    spread = jnp.where(walker_ids == low + offset, column, spread)
                wide[here, :] = spread
            block = map_ref[here, :]
            current = dot(block, term[...], CONTRACT_LAST).astype(jnp.bfloat16)
            scaled = (wide[here, :] * current.astype(jnp.float32)).astype(jnp.bfloat16)
            total[...] += dot(scaled, block, CONTRACT_FIRST)

        term[...] = (total[...] / degree).astype(jnp.bfloat16)
        running = running + term[...].astype(jnp.float32)
    out_ref[...] = running.astype(jnp.bfloat16)


def propagate(n, occupied, map_full, field_full, own_cols_t):
    points, orbitals = map_full.shape
    own = own_cols_t.shape[0]
    piece = next(p for p in (1280, 640, 256, points // n) if points % p == 0)
    return pl.pallas_call(
        functools.partial(propagate_kernel, n, occupied, piece),
        out_shape=jax.ShapeDtypeStruct((own, orbitals), jnp.bfloat16),
        in_specs=[pl.BlockSpec(memory_space=pltpu.VMEM)] * 3,
        out_specs=pl.BlockSpec(memory_space=pltpu.VMEM),
        scratch_shapes=[
            pltpu.VMEM((points, own), jnp.float32),
            pltpu.VMEM((own, orbitals), jnp.float32),
            pltpu.VMEM((own, orbitals), jnp.bfloat16),
        ],
        cost_estimate=pl.CostEstimate(
            flops=12 * points * orbitals * own, bytes_accessed=2 * map_full.size, transcendentals=0
        ),
        compiler_params=pltpu.CompilerParams(vmem_limit_bytes=60 * 2**20),
        name="propagate",
    )(map_full, field_full, own_cols_t)


def exchange_plain(trial, trial_here, core, orbit):
    core_block = core.astype(jnp.float32)

    def per_walker(operands):
        left_orb, right_orb = operands
        forward = jnp.dot(left_orb, trial.T, preferred_element_type=jnp.float32)
        backward = jnp.dot(trial_here, right_orb.T, preferred_element_type=jnp.float32)
        return jnp.sum(core_block * forward * backward)

    everyone = lax.all_gather(orbit, "pts", axis=0, tiled=True)
    return lax.map(per_walker, (jnp.moveaxis(orbit, 1, 0), jnp.moveaxis(everyone, 1, 0)))


def body(points_map, trial, core, walkers, draws):
    point_rows = points_map.shape[0]
    orbitals = points_map.shape[1]
    walker_count = walkers.shape[1]
    occupied = walkers.shape[2]
    n = lax.axis_size("pts")
    point_first = lax.axis_index("pts") * point_rows
    trial_here = lax.dynamic_slice_in_dim(trial, point_first, point_rows, 0)
    flat_walkers = walkers.reshape(orbitals, walker_count * occupied)
    flat_orbit = jnp.dot(points_map, flat_walkers, preferred_element_type=jnp.float32).astype(jnp.bfloat16)
    orbit = flat_orbit.reshape(point_rows, walker_count, occupied)
    density = (
        jnp.sum(orbit.astype(jnp.float32) * trial_here.astype(jnp.float32)[:, None, :], axis=2)
        / math.sqrt(occupied)
    ).astype(jnp.bfloat16)
    potential = jnp.dot(
        core,
        lax.all_gather(density, "pts", axis=0, tiled=True),
        preferred_element_type=jnp.float32,
    )
    field = FIELD_STEP * (node_lookup(draws) - FIELD_STEP * potential)
    field_full = lax.all_gather(field, "pts", axis=0, tiled=True)
    own_rows = orbitals // n
    own_cols = walker_count * occupied // n
    col_start = lax.axis_index("pts") * own_cols
    cols_walkers = lax.dynamic_slice_in_dim(flat_walkers, col_start, own_cols, 1)
    if point_rows % 16 == 0 and n % 8 == 0:
        sums, final_t = fused(
            n, points_map, trial, trial_here, core, flat_walkers, flat_orbit, field_full, cols_walkers.T, walker_count
        )
        exchange = jnp.sum(sums, axis=(1, 2))
    else:
        map_full = lax.all_gather(points_map, "pts", axis=0, tiled=True)
        final_t = propagate(n, occupied, map_full, field_full, cols_walkers.T)
        exchange = exchange_plain(trial, trial_here, core, orbit)
    placed = lax.all_to_all(final_t.T, "pts", split_axis=0, concat_axis=1, tiled=True)
    hartree = jnp.sum(density.astype(jnp.float32) * potential, axis=0)
    total_points = point_rows * n
    energy = lax.psum((hartree - exchange / occupied) / (2.0 * total_points), "pts")
    return (placed.reshape(own_rows, walker_count, occupied), energy)


def solution(mesh):
    placed = (
        P(("mol", "pts"), None),
        P("mol", None),
        P(("mol", "pts"), None),
        P("mol", None, None),
        P(("mol", "pts"), None),
    )
    return jax.shard_map(
        body,
        mesh=mesh,
        in_specs=placed,
        out_specs=(P(("mol", "pts"), None, None), P("mol")),
        check_vma=False,
    )
```

```python
import functools
import math

import jax
import jax.numpy as jnp
from jax import lax
from jax.experimental import pallas as pl
from jax.experimental.pallas import tpu as pltpu
from jax.sharding import PartitionSpec as P

TAYLOR = 3


GAUSS_NODES = (-2.3344142, -0.7419637, 0.7419637, 2.3344142)
FIELD_STEP = 0.15
LANES = 128
CONTRACT_LAST = (((1,), (1,)), ((), ()))
CONTRACT_FIRST = (((0,), (0,)), ((), ()))


def node_lookup(draws):
    values = jnp.zeros(draws.shape, jnp.float32)
    for number, node in enumerate(GAUSS_NODES):
        values = values + jnp.where(draws == number, node, 0.0).astype(jnp.float32)
    return values


def dot(left, right, dims):
    return lax.dot_general(left, right, dims, preferred_element_type=jnp.float32)


def add_exchange(out_ref, blocks, map_block, trial_ref, trial_own, core_ref, walkers_ref, orbit_own, first, weight):
    rows, occupied = trial_own.shape
    window = blocks.shape[0]
    base = pl.multiple_of(first // LANES * LANES, LANES)
    shift = pl.multiple_of(first - base, 16)
    blocks[...] = jnp.zeros_like(blocks)
    blocks[pl.ds(shift, rows), :] = dot(map_block, walkers_ref[...], (((1,), (0,)), ((), ()))).astype(jnp.bfloat16)
    core_here = core_ref[:, pl.ds(base, window)].astype(jnp.float32)
    trial_there = trial_ref[pl.ds(base, window), :]
    for walker in range(out_ref.shape[0]):
        cols = slice(walker * occupied, (walker + 1) * occupied)
        forward = dot(orbit_own[:, cols], trial_there, CONTRACT_LAST)
        backward = dot(trial_own[...], blocks[:, cols], CONTRACT_LAST)
        product = core_here * forward * backward
        out_ref[walker] += weight * jnp.sum(product.reshape(rows // 8, 8, window), axis=0)


def spread_field(field_ref, here, piece, start, own, occupied):
    walker_ids = (start + lax.broadcasted_iota(jnp.int32, (1, own), 1)) // occupied
    low = start // occupied
    field = field_ref[here, :]
    lane = lax.broadcasted_iota(jnp.int32, field.shape, 1)
    spread = jnp.zeros((piece, own), jnp.float32)
    for offset in range((own + occupied - 2) // occupied + 1):
        column = jnp.sum(jnp.where(lane == low + offset, field, 0.0), axis=1, keepdims=True)
        spread = jnp.where(walker_ids == low + offset, column, spread)
    return spread


def fused_kernel(
    n, piece, own_map, trial_ref, trial_own, core_ref, walkers_ref, orbit_own, field_ref, cols_ref,
    sums_ref, out_ref,
    blocks, gathered, wide, total, term, right_sems, left_sems, side_sems, recv_sems,
):
    rows, occupied = trial_own.shape
    own = cols_ref.shape[0]
    points = gathered.shape[0]
    chips = n // 2
    far = chips // 2
    top = (rows // 2 + 15) // 16 * 16
    parts = ((0, top), (top, rows - top))
    me = lax.axis_index("pts")
    core_id = lax.rem(me, 2)
    chip = me // 2
    ring = jnp.where(lax.rem(chip, 2) == 0, chip // 2, chips - 1 - chip // 2)

    def device(place, side):
        place = lax.rem(place + 2 * chips, chips)
        where = jnp.where(place < far, 2 * place, 2 * (chips - 1 - place) + 1)
        return 2 * where + side

    right, left, partner = device(ring + 1, core_id), device(ring - 1, core_id), device(ring, 1 - core_id)

    def slot(index, part=None):
        offset, length = (0, rows) if part is None else parts[part]
        return gathered.at[pl.ds(pl.multiple_of(index * rows + offset, 16), length), :]

    def send(src, index, part, send_sem, target):
        return pltpu.make_async_remote_copy(
            src_ref=src,
            dst_ref=slot(index, part),
            send_sem=send_sem,
            recv_sem=recv_sems.at[index, part or 0],
            device_id={"pts": target},
            device_id_type=pl.DeviceIdType.MESH,
        )

    def forward(index, part, send_sem, target):
        send(slot(index, part), index, part, send_sem, target).start()

    def arrived(index, part=None):
        send(slot(index, part), index, part, side_sems.at[0, 0], partner).wait_recv()

    barrier = pltpu.get_barrier_semaphore()
    for other in (right, left, partner):
        pl.semaphore_signal(barrier, inc=1, device_id={"pts": other}, device_id_type=pl.DeviceIdType.MESH)
    pl.semaphore_wait(barrier, 3)
    send(own_map, me, None, right_sems.at[0], right).start()
    send(own_map, me, None, left_sems.at[0], left).start()
    send(own_map, me, None, side_sems.at[0, 0], partner).start()
    gathered[pl.ds(pl.multiple_of(me * rows, 16), rows), :] = own_map[...]
    sums_ref[...] = jnp.zeros_like(sums_ref)
    total[...] = jnp.zeros_like(total)
    term[...] = cols_ref[...]

    def add_block(index):
        here = pl.ds(pl.multiple_of(index * rows, 16), rows)
        block = gathered[here, :]
        spread = spread_field(field_ref, here, rows, me * own, own, occupied)
        wide[here, :] = spread
        current = dot(block, term[...], CONTRACT_LAST).astype(jnp.bfloat16)
        scaled = (spread * current.astype(jnp.float32)).astype(jnp.bfloat16)
        total[...] += dot(scaled, block, CONTRACT_FIRST)

    @pl.loop(0, 2 * far + 1)
    def _(task):
        hop = task // 2
        same = lax.rem(task, 2) == 0
        ahead, behind = device(ring + hop, core_id), device(ring - hop, core_id)
        ahead_side, behind_side = device(ring + hop, 1 - core_id), device(ring - hop, 1 - core_id)
        last = hop == far
        middle = jnp.logical_and(hop > 0, hop < far)

        @pl.when(jnp.logical_and(same, middle))
        def _():
            arrived(behind)

            @pl.when(hop < far - 1)
            def _():
                forward(behind, None, right_sems.at[hop], right)

            @pl.when(hop == far - 1)
            def _():
                forward(behind, 0, right_sems.at[hop], right)

            forward(behind, None, side_sems.at[0, hop], partner)
            arrived(ahead)

            @pl.when(hop < far - 1)
            def _():
                forward(ahead, None, left_sems.at[hop], left)

            @pl.when(hop == far - 1)
            def _():
                forward(ahead, 1, left_sems.at[hop], left)

            forward(ahead, None, side_sems.at[1, hop], partner)

        @pl.when(last)
        def _():
            for part in range(2):
                arrived(ahead, part)
                forward(ahead, part, side_sems.at[part, hop], partner)
            for part in range(2):
                arrived(ahead_side, part)

        @pl.when(jnp.logical_not(same))
        def _():
            arrived(ahead_side)

            @pl.when(hop > 0)
            def _():
                arrived(behind_side)

        near = jnp.where(same, ahead, ahead_side)
        opposite = jnp.where(last, ahead_side, jnp.where(same, behind, behind_side))
        pair = jnp.where(jnp.logical_and(last, ring >= far), ahead_side, near)
        add_exchange(
            sums_ref, blocks, gathered[pl.ds(pl.multiple_of(pair * rows, 16), rows), :], trial_ref, trial_own,
            core_ref, walkers_ref, orbit_own, pair * rows, jnp.where(hop == 0, 1.0, 2.0),
        )
        add_block(near)

        @pl.when(hop > 0)
        def _():
            add_block(opposite)

    running = cols_ref[...].astype(jnp.float32)
    for degree in range(1, TAYLOR + 1):
        if degree > 1:
            total[...] = jnp.zeros_like(total)

            @pl.loop(0, points // piece)
            def _(number):
                here = pl.ds(pl.multiple_of(number * piece, piece), piece)
                block = gathered[here, :]
                current = dot(block, term[...], CONTRACT_LAST).astype(jnp.bfloat16)
                scaled = (wide[here, :] * current.astype(jnp.float32)).astype(jnp.bfloat16)
                total[...] += dot(scaled, block, CONTRACT_FIRST)

        term[...] = (total[...] / degree).astype(jnp.bfloat16)
        running = running + term[...].astype(jnp.float32)
    out_ref[...] = running.astype(jnp.bfloat16)

    for hop in range(far):
        for number, (sems, target) in enumerate(((right_sems, right), (left_sems, left))):
            part = number if hop == far - 1 and hop > 0 else None
            send(slot(me, part), me, part, sems.at[hop], target).wait_send()
    send(slot(me), me, None, side_sems.at[0, 0], partner).wait_send()
    for hop in range(1, far + 1):
        for number in range(2):
            part = number if hop == far else None
            send(slot(me, part), me, part, side_sems.at[number, hop], partner).wait_send()


def fused(n, points_map, trial, trial_here, core, flat_walkers, orbit, field_full, own_cols_t, walker_count):
    rows, orbitals = points_map.shape
    points, own, columns = rows * n, own_cols_t.shape[0], flat_walkers.shape[1]
    window = (rows + (LANES - 16) + LANES - 1) // LANES * LANES
    far = n // 4
    piece = next(p for p in (1280, 640, 256, rows) if points % p == 0)
    dma = pltpu.SemaphoreType.DMA
    return pl.pallas_call(
        functools.partial(fused_kernel, n, piece),
        out_shape=(
            jax.ShapeDtypeStruct((walker_count, 8, window), jnp.float32),
            jax.ShapeDtypeStruct((own, orbitals), jnp.bfloat16),
        ),
        in_specs=[pl.BlockSpec(memory_space=pltpu.VMEM)] * 8,
        out_specs=[pl.BlockSpec(memory_space=pltpu.VMEM)] * 2,
        scratch_shapes=[
            pltpu.VMEM((window, columns), jnp.bfloat16),
            pltpu.VMEM((points, orbitals), jnp.bfloat16),
            pltpu.VMEM((points, own), jnp.float32),
            pltpu.VMEM((own, orbitals), jnp.float32),
            pltpu.VMEM((own, orbitals), jnp.bfloat16),
            dma((far,)),
            dma((far,)),
            dma((2, far + 1)),
            dma((n, 2)),
        ],
        compiler_params=pltpu.CompilerParams(
            collective_id=0, has_side_effects=True, vmem_limit_bytes=60 * 2**20
        ),
        name="fused",
    )(points_map, trial, trial_here, core, flat_walkers, orbit, field_full, own_cols_t)


def propagate_kernel(n, occupied, piece, map_ref, field_ref, cols_ref, out_ref, wide, total, term):
    points, orbitals = map_ref.shape
    own = cols_ref.shape[0]
    start = lax.axis_index("pts") * own
    walker_ids = (start + lax.broadcasted_iota(jnp.int32, (1, own), 1)) // occupied
    low = start // occupied
    span = (own + occupied - 2) // occupied + 1
    running = cols_ref[...].astype(jnp.float32)
    term[...] = cols_ref[...]
    for degree in range(1, TAYLOR + 1):
        total[...] = jnp.zeros_like(total)

        @pl.loop(0, points // piece)
        def _(number):
            here = pl.ds(pl.multiple_of(number * piece, piece), piece)
            if degree == 1:
                field = field_ref[here, :]
                lane = lax.broadcasted_iota(jnp.int32, field.shape, 1)
                spread = jnp.zeros((piece, own), jnp.float32)
                for offset in range(span):
                    column = jnp.sum(jnp.where(lane == low + offset, field, 0.0), axis=1, keepdims=True)
                    spread = jnp.where(walker_ids == low + offset, column, spread)
                wide[here, :] = spread
            block = map_ref[here, :]
            current = dot(block, term[...], CONTRACT_LAST).astype(jnp.bfloat16)
            scaled = (wide[here, :] * current.astype(jnp.float32)).astype(jnp.bfloat16)
            total[...] += dot(scaled, block, CONTRACT_FIRST)

        term[...] = (total[...] / degree).astype(jnp.bfloat16)
        running = running + term[...].astype(jnp.float32)
    out_ref[...] = running.astype(jnp.bfloat16)


def propagate(n, occupied, map_full, field_full, own_cols_t):
    points, orbitals = map_full.shape
    own = own_cols_t.shape[0]
    piece = next(p for p in (1280, 640, 256, points // n) if points % p == 0)
    return pl.pallas_call(
        functools.partial(propagate_kernel, n, occupied, piece),
        out_shape=jax.ShapeDtypeStruct((own, orbitals), jnp.bfloat16),
        in_specs=[pl.BlockSpec(memory_space=pltpu.VMEM)] * 3,
        out_specs=pl.BlockSpec(memory_space=pltpu.VMEM),
        scratch_shapes=[
            pltpu.VMEM((points, own), jnp.float32),
            pltpu.VMEM((own, orbitals), jnp.float32),
            pltpu.VMEM((own, orbitals), jnp.bfloat16),
        ],
        cost_estimate=pl.CostEstimate(
            flops=12 * points * orbitals * own, bytes_accessed=2 * map_full.size, transcendentals=0
        ),
        compiler_params=pltpu.CompilerParams(vmem_limit_bytes=60 * 2**20),
        name="propagate",
    )(map_full, field_full, own_cols_t)


def exchange_plain(trial, trial_here, core, orbit):
    core_block = core.astype(jnp.float32)

    def per_walker(operands):
        left_orb, right_orb = operands
        forward = jnp.dot(left_orb, trial.T, preferred_element_type=jnp.float32)
        backward = jnp.dot(trial_here, right_orb.T, preferred_element_type=jnp.float32)
        return jnp.sum(core_block * forward * backward)

    everyone = lax.all_gather(orbit, "pts", axis=0, tiled=True)
    return lax.map(per_walker, (jnp.moveaxis(orbit, 1, 0), jnp.moveaxis(everyone, 1, 0)))


def gather_stacked(part):
    n = lax.axis_size("pts")
    copies = jnp.broadcast_to(part[None], (n,) + part.shape)
    return lax.all_to_all(copies, "pts", split_axis=0, concat_axis=0, tiled=True)


def body(points_map, trial, core, walkers, draws):
    point_rows = points_map.shape[0]
    orbitals = points_map.shape[1]
    walker_count = walkers.shape[1]
    occupied = walkers.shape[2]
    n = lax.axis_size("pts")
    point_first = lax.axis_index("pts") * point_rows
    trial_here = lax.dynamic_slice_in_dim(trial, point_first, point_rows, 0)
    flat_walkers = walkers.reshape(orbitals, walker_count * occupied)
    flat_orbit = jnp.dot(points_map, flat_walkers, preferred_element_type=jnp.float32).astype(jnp.bfloat16)
    orbit = flat_orbit.reshape(point_rows, walker_count, occupied)
    density = (
        jnp.sum(orbit.astype(jnp.float32) * trial_here.astype(jnp.float32)[:, None, :], axis=2)
        / math.sqrt(occupied)
    ).astype(jnp.bfloat16)
    potential = jnp.dot(
        core,
        jnp.moveaxis(gather_stacked(density.T), 2, 1).reshape(point_rows * n, walker_count),
        preferred_element_type=jnp.float32,
    )
    field = FIELD_STEP * (node_lookup(draws) - FIELD_STEP * potential)
    field_full = jnp.moveaxis(gather_stacked(field.T), 2, 1).reshape(point_rows * n, walker_count)
    own_rows = orbitals // n
    own_cols = walker_count * occupied // n
    col_start = lax.axis_index("pts") * own_cols
    cols_walkers = lax.dynamic_slice_in_dim(flat_walkers, col_start, own_cols, 1)
    if point_rows % 16 == 0 and n % 8 == 0:
        sums, final_t = fused(
            n, points_map, trial, trial_here, core, flat_walkers, flat_orbit, field_full, cols_walkers.T, walker_count
        )
        exchange = jnp.sum(sums, axis=(1, 2))
    else:
        map_full = lax.all_gather(points_map, "pts", axis=0, tiled=True)
        final_t = propagate(n, occupied, map_full, field_full, cols_walkers.T)
        exchange = exchange_plain(trial, trial_here, core, orbit)
    placed = lax.all_to_all(final_t.T, "pts", split_axis=0, concat_axis=1, tiled=True)
    hartree = jnp.sum(density.astype(jnp.float32) * potential, axis=0)
    total_points = point_rows * n
    energy = jnp.sum(gather_stacked((hartree - exchange / occupied) / (2.0 * total_points)), axis=0)
    return (placed.reshape(own_rows, walker_count, occupied), energy)


def solution(mesh):
    placed = (
        P(("mol", "pts"), None),
        P("mol", None),
        P(("mol", "pts"), None),
        P("mol", None, None),
        P(("mol", "pts"), None),
    )
    return jax.shard_map(
        body,
        mesh=mesh,
        in_specs=placed,
        out_specs=(P(("mol", "pts"), None, None), P("mol")),
        check_vma=False,
    )
```
